768 devices in a mesh: section: 4 (over x_lo, core), shard: 8 (over y), replica: 24 (over z, x_hi).
Axes of the slice: x: 4 (x_hi: 2, x_lo: 2; x = x_hi * 2 + x_lo), y: 8, z: 12, core: 2. Of those that a mesh axis runs over, the one named last changes fastest.
Arguments:
- acts_fwd: bfloat16 [4, 24576, 4096], P('section', ('shard', 'replica')), may hold values from -30 to 30
- pos_fwd: int32 [4, 24576], P('section', ('shard', 'replica')), may hold values from 0 to 2047
- saved_acts: bfloat16 [4, 24576, 4096], P('section', ('shard', 'replica')), may hold values from -30 to 30
- pos_bwd: int32 [4, 24576], P('section', ('shard', 'replica')), may hold values from 0 to 2047
- grads_in: bfloat16 [4, 24576, 4096], P('section', ('shard', 'replica')), may hold values from -6 to 6
- key_cotan: bfloat16 [4, 24576, 512], P('section', ('shard', 'replica')), may hold values from -6 to 6
- weight: bfloat16 [4, 4096, 512], P('section', 'shard'), may hold values from -0.09375 to 0.09375
- gain: float32 [4, 4096], P('section'), may hold values from 0.1 to 1.9
Outputs:
- keys: bfloat16 [4, 24576, 512], P('section', ('shard', 'replica'))
- grad_out: bfloat16 [4, 24576, 4096], P('section', ('shard', 'replica'))
- weight_grad: float32 [4, 4096, 512], P('section', 'shard')
The draws below stay inside these ranges and needn't reach their ends.
All inputs are finite; a program needn't handle non-finite values.
Results may differ from the reference program's by a relative error of at most 0.0058.
Values may be sent and summed in bfloat16 or wider, within the bound.
No kernel may reach another device: no remote copies, remote signals or barrier semaphores. Data moves between devices by JAX's collectives and lax.ppermute only.
A program may use at most 64 MiB of HBM per device.

```python
import math
import jax
import jax.numpy as jnp
from jax import lax

D = 4096
HEAD = 128
KVH = 4
SEQ = 2048
TOK_DEV = 128
TOKENS = 24576
N_SECTION = 4


def rough_rows(key):
    shape = (N_SECTION, TOKENS, D)
    scale_key = jax.random.fold_in(key, 11)
    base_key = jax.random.fold_in(key, 12)
    scales = jnp.exp(jax.random.uniform(scale_key, (N_SECTION, TOKENS, 1), jnp.float32, math.log(0.5), math.log(5.0)))
    base = jnp.clip(jax.random.normal(base_key, shape, jnp.float32), -5.0, 5.0)
    values = base * scales
    return jnp.clip(values, -30.0, 30.0).astype(jnp.bfloat16)


def draw_acts_fwd(key, part):
    return rough_rows(jax.random.fold_in(key, 101))


def draw_saved_acts(key, part):
    return rough_rows(jax.random.fold_in(key, 202))


def plant(entries, own_key, smallest, top_value):
    shape = entries.shape
    index_at = [jax.random.randint(jax.random.fold_in(own_key, axis), (), 0, shape[axis]) for axis in range(len(shape))]
    entries = entries.at[tuple(index_at)].set(smallest)
    longest = shape.index(max(shape))
    index_at[longest] = (index_at[longest] + 1) % shape[longest]
    return entries.at[tuple(index_at)].set(top_value)


def levels(key, shape, pieces, low, largest):
    def one(axis_at, shards_of):
        heights = jax.random.uniform(jax.random.fold_in(jax.random.fold_in(key, 6), axis_at), (shards_of,), jnp.float32, low / len(pieces), largest / len(pieces))
        return jnp.repeat(jnp.exp(heights), shape[axis_at] // shards_of).reshape((-1,) + (1,) * (len(shape) - axis_at - 1))

    factor_of = one(*pieces[0])
    for cut in pieces[1:]:
        factor_of = factor_of * one(*cut)
    return factor_of


def noise(own_key, extent, width, limit, split=(), kind=jnp.bfloat16):
    values = width * jax.random.normal(own_key, extent, jnp.float32)
    if split:
        values = values * levels(own_key, extent, split, -0.22, 0.18)
    return jnp.clip(values, -limit, limit).astype(kind)


def setup_inputs(seed: int = 0) -> dict:
    key_list = jax.random.split(jax.random.key(seed), 9)
    acts_fwd = draw_acts_fwd(jax.random.fold_in(key_list[8], 71), 0)
    pos_fwd = plant(jax.random.randint(key_list[1], (N_SECTION, TOKENS), 0, SEQ), jax.random.fold_in(key_list[1], 1), 0, SEQ - 1).astype(jnp.int32)
    saved_acts = draw_saved_acts(jax.random.fold_in(key_list[8], 71), 0)
    pos_bwd = plant(jax.random.randint(key_list[3], (N_SECTION, TOKENS), 0, SEQ), jax.random.fold_in(key_list[3], 1), 0, SEQ - 1).astype(jnp.int32)
    grads_in = noise(key_list[4], (N_SECTION, TOKENS, D), 1.0, 6.0, ((0, 4), (1, 192)))
    key_cotan = noise(key_list[5], (N_SECTION, TOKENS, KVH * HEAD), 1.0, 6.0, ((0, 4), (1, 192)))
    weight = noise(key_list[6], (N_SECTION, D, KVH * HEAD), D ** -0.5, 0.09375, ((0, 4), (1, 8)))
    gain = jnp.clip(1.0 + 0.18 * jax.random.normal(key_list[7], (N_SECTION, D), jnp.float32), 0.1, 1.9)
    return dict(acts_fwd=acts_fwd, pos_fwd=pos_fwd, saved_acts=saved_acts, pos_bwd=pos_bwd, grads_in=grads_in, key_cotan=key_cotan, weight=weight, gain=gain)


def rope_tables(positions):
    index = jnp.arange(HEAD // 2, dtype=jnp.float32)
    rate = 500000.0 ** (-(2.0 * index) / HEAD)
    angle = positions.astype(jnp.float32)[:, None] * rate[None, :]
    return (jnp.cos(angle), jnp.sin(angle))

def rotate(values, cosine, sine_part, orient):
    count = values.shape[0]
    shaped = values.reshape(count, KVH, HEAD)
    first_half = shaped[..., :HEAD // 2]
    second_half = shaped[..., HEAD // 2:]
    cos_b = cosine[:, None, :]
    sin_b = orient * sine_part[:, None, :]
    joined = jnp.concatenate([first_half * cos_b - second_half * sin_b, second_half * cos_b + first_half * sin_b], -1)
    return joined.reshape(count, KVH * HEAD)

def normalize(stream, gain_row):
    values = stream.astype(jnp.float32)
    inverse = lax.rsqrt(lax.optimization_barrier(jnp.mean(values * values, -1, keepdims=True)) + 1e-05)
    return (values * inverse * gain_row[None, :], inverse, values)

def one_section(packed):
    stream, pos_f, saved, pos_b, arrived, cotan, proj, gain_row = packed
    normed = normalize(stream, gain_row)[0].astype(jnp.bfloat16)
    projected = jnp.dot(normed, proj, preferred_element_type=jnp.float32)
    cosine, sine_part = rope_tables(pos_f)
    keys = rotate(projected, cosine, sine_part, 1.0).astype(jnp.bfloat16)
    back_f, inverse, saved_f = normalize(saved, gain_row)
    back_normed = back_f.astype(jnp.bfloat16)
    cos_b, sin_b = rope_tables(pos_b)
    key_grad = rotate(cotan.astype(jnp.float32), cos_b, sin_b, -1.0).astype(jnp.bfloat16)
    normed_grad = jnp.dot(key_grad, proj.T, preferred_element_type=jnp.float32)
    scaled = normed_grad * gain_row[None, :]
    stream_grad = inverse * scaled - saved_f * inverse ** 3 * lax.optimization_barrier(jnp.mean(saved_f * scaled, -1, keepdims=True))
    grad_out = (arrived.astype(jnp.float32) + stream_grad).astype(jnp.bfloat16)
    blocks = TOKENS // TOK_DEV
    norm_blocks = back_normed.reshape(blocks, TOK_DEV, D)
    grad_blocks = key_grad.reshape(blocks, TOK_DEV, KVH * HEAD)

    def accumulate(total, pair):
        term = lax.dot_general(pair[0], pair[1], (((0,), (0,)), ((), ())), preferred_element_type=jnp.float32)
        rounded = lax.optimization_barrier(term.astype(jnp.bfloat16))
        return (total + rounded.astype(jnp.float32), None)
    start = jnp.zeros((D, KVH * HEAD), jnp.float32)
    total, unused = lax.scan(accumulate, start, (norm_blocks, grad_blocks))
    weight_grad = total * float(TOKENS) ** (-0.5)
    return (keys, grad_out, weight_grad)

def reference(acts_fwd, pos_fwd, saved_acts, pos_bwd, grads_in, key_cotan, weight, gain):
    streams = jnp.concatenate([acts_fwd[:1], acts_fwd[:-1]], 0)
    arrivals = jnp.concatenate([grads_in[1:], grads_in[-1:]], 0)
    keys, grad_out, weight_grad = lax.map(one_section, (streams, pos_fwd, saved_acts, pos_bwd, arrivals, key_cotan, weight, gain))
    return (keys, grad_out, weight_grad)
```

```python
import jax
import jax.numpy as jnp
from jax import lax
from jax.sharding import PartitionSpec as P


HEAD = 128
LANES = 128


def from_behind(x, axis, by):
    size = lax.axis_size(axis)
    pairs = [(i, i + by) for i in range(size) if 0 <= i + by < size]
    return lax.ppermute(x, axis, pairs)


def rope_tables(positions):
    index = jnp.arange(HEAD // 2, dtype=jnp.float32)
    rate = 500000.0 ** (-(2.0 * index) / HEAD)
    angle = positions.astype(jnp.float32)[:, None] * rate[None, :]
    return (jnp.cos(angle), jnp.sin(angle))


def rotate(values, cosine, sine_part, orient):
    cos_full = jnp.concatenate([cosine, cosine], -1)
    sin_full = jnp.concatenate([-orient * sine_part, orient * sine_part], -1)
    heads = []
    for start in range(0, values.shape[1], HEAD):
        head = values[:, start : start + HEAD]
        swapped = jnp.concatenate([head[:, HEAD // 2 :], head[:, : HEAD // 2]], -1)
        heads.append(head * cos_full + swapped * sin_full)
    return jnp.concatenate(heads, -1)


def normalize(stream, gain_row):
    values = stream.astype(jnp.float32)
    inverse = lax.rsqrt(jnp.mean(values * values, -1, keepdims=True) + 1e-05)
    return (values * inverse * gain_row[None, :], inverse, values)


def swap_shards(rows):
    count = lax.axis_size("shard")
    tokens, width = rows.shape
    pieces = rows.reshape(tokens, count, width // count).transpose(1, 0, 2)
    return lax.all_to_all(pieces, "shard", split_axis=0, concat_axis=0).reshape(count * tokens, width // count)


def sum_over_replicas(term):
    rows, cols = term.shape
    count = lax.axis_size("replica")
    tall = term.astype(jnp.bfloat16).reshape(rows, cols // LANES, LANES).transpose(1, 0, 2).reshape(-1, LANES)
    total = tall.shape[0]
    piece = -(-total // (count * 8)) * 8
    tall = jnp.pad(tall, ((0, piece * count - total), (0, 0))).reshape(count, piece, LANES)
    got = lax.all_to_all(tall, "replica", split_axis=0, concat_axis=0)
    own = jnp.sum(got.astype(jnp.float32), 0).astype(jnp.bfloat16)
    full = lax.all_to_all(jnp.broadcast_to(own[None], (count, piece, LANES)), "replica", split_axis=0, concat_axis=0)
    full = full.reshape(count * piece, LANES)[:total].astype(jnp.float32)
    return full.reshape(cols // LANES, rows, LANES).transpose(1, 0, 2).reshape(rows, cols)


def per_device(acts_fwd, pos_fwd, saved_acts, pos_bwd, grads_in, key_cotan, weight, gain):
    section_pos = lax.axis_index("section")
    section_count = lax.axis_size("section")
    shard_count = lax.axis_size("shard")
    replica_count = lax.axis_size("replica")
    tok_rows = saved_acts.shape[1]
    gain_row = gain[0]
    local_rows = weight[0]
    saved_cols = swap_shards(saved_acts[0])
    saved_f = saved_acts[0].astype(jnp.float32)
    inverse = lax.rsqrt(jnp.mean(saved_f * saved_f, -1, keepdims=True) + 1e-05)
    cos_b, sin_b = rope_tables(pos_bwd[0])
    key_grad_f = rotate(key_cotan[0].astype(jnp.float32), cos_b, sin_b, -1.0)
    key_grad = key_grad_f.astype(jnp.bfloat16)
    own_keys, local_rows = lax.optimization_barrier(
        ((key_grad_f * inverse).astype(jnp.bfloat16), local_rows)
    )
    scaled_keys = lax.all_gather(own_keys, "shard", axis=0, tiled=True)
    gathered = lax.all_gather(local_rows, "shard", axis=0, tiled=True)
    term = lax.dot_general(
        saved_cols, scaled_keys, (((0,), (0,)), ((), ())), preferred_element_type=jnp.float32
    )
    summed = sum_over_replicas(term)
    own_rows = local_rows.shape[0]
    own_gain = lax.dynamic_slice(gain_row, (lax.axis_index("shard") * own_rows,), (own_rows,))
    token_total = tok_rows * shard_count * replica_count
    weight_grad = summed * (own_gain * float(token_total) ** (-0.5))[:, None]
    came_fwd = from_behind(acts_fwd, "section", 1)
    stream = jnp.where(section_pos == 0, acts_fwd, came_fwd)[0]
    came_bwd = from_behind(grads_in, "section", -1)
    arrived = jnp.where(section_pos == section_count - 1, grads_in, came_bwd)[0]
    normed = normalize(stream, gain_row)[0].astype(jnp.bfloat16)
    projected = jnp.dot(normed, gathered, preferred_element_type=jnp.float32)
    normed_grad = lax.dot_general(
        key_grad, gathered, (((1,), (1,)), ((), ())), preferred_element_type=jnp.float32
    )
    cosine, sine_part = rope_tables(pos_fwd[0])
    keys = rotate(projected, cosine, sine_part, 1.0).astype(jnp.bfloat16)
    scaled = normed_grad * gain_row[None, :]
    stream_grad = inverse * scaled - saved_f * inverse**3 * jnp.mean(
        saved_f * scaled, -1, keepdims=True
    )
    grad_out = (arrived.astype(jnp.float32) + stream_grad).astype(jnp.bfloat16)
    return (keys[None], grad_out[None], weight_grad[None])


def solution(mesh):
    placed = (
        P("section", ("shard", "replica"), None),
        P("section", ("shard", "replica")),
        P("section", ("shard", "replica"), None),
        P("section", ("shard", "replica")),
        P("section", ("shard", "replica"), None),
        P("section", ("shard", "replica"), None),
        P("section", "shard", None),
        P("section", None),
    )

    return jax.shard_map(
        per_device,
        mesh=mesh,
        in_specs=placed,
        out_specs=(
            P("section", ("shard", "replica"), None),
            P("section", ("shard", "replica"), None),
            P("section", "shard", None),
        ),
        check_vma=False,
    )
```

```python
import jax
import jax.numpy as jnp
from jax import lax
from jax.experimental import pallas as pl
from jax.experimental.pallas import tpu as pltpu
from jax.sharding import PartitionSpec as P


HEAD = 128
LANES = 128
EPS = 1e-05
F32 = jnp.float32
BF16 = jnp.bfloat16


def from_behind(x, axis, by):
    size = lax.axis_size(axis)
    pairs = [(i, i + by) for i in range(size) if 0 <= i + by < size]
    return lax.ppermute(x, axis, pairs)


def rope_tables(positions):
    index = jnp.arange(HEAD // 2, dtype=F32)
    rate = 500000.0 ** (-(2.0 * index) / HEAD)
    rate = jnp.concatenate([rate, rate])
    sign = jnp.where(jnp.arange(HEAD) < HEAD // 2, -1.0, 1.0).astype(F32)
    angle = positions.astype(F32)[:, None] * rate[None, :]
    return jnp.cos(angle), jnp.sin(angle) * sign[None, :]


def turn(head, cosine, sine_part):
    return head * cosine + pltpu.roll(head, HEAD // 2, 1) * sine_part


def keys_kernel(saved_ref, cotan_ref, cos_ref, sin_ref, grad_ref, scaled_ref):
    saved = saved_ref[...].astype(F32)
    inverse = lax.rsqrt(jnp.mean(saved * saved, -1, keepdims=True) + EPS)
    cosine = cos_ref[...]
    sine_part = -sin_ref[...]
    for start in range(0, cotan_ref.shape[1], HEAD):
        span = pl.ds(start, HEAD)
        turned = turn(cotan_ref[:, span].astype(F32), cosine, sine_part)
        grad_ref[:, span] = turned.astype(BF16)
        scaled_ref[:, span] = (turned * inverse).astype(BF16)


def key_factors(saved, cotan, cosine, sine_part):
    shape = jax.ShapeDtypeStruct(cotan.shape, BF16)
    return pl.pallas_call(keys_kernel, out_shape=(shape, shape), name="key_factors")(saved, cotan, cosine, sine_part)


def term_kernel(shard_ref, saved_ref, *rest):
    *key_refs, out_ref, acc_ref = rest
    count = saved_ref.shape[0]
    for place, key_ref in enumerate(key_refs):
        distance, first = RING[place]
        block = lax.rem(shard_ref[0] + count - distance, count)
        part = saved_ref[block, pl.ds(first, key_ref.shape[0]), :]
        term = lax.dot_general(part, key_ref[...], (((0,), (0,)), ((), ())), preferred_element_type=F32)
        if place == 0:
            acc_ref[...] = term
        else:
            acc_ref[...] += term
    rows, cols = acc_ref.shape
    for block in range(cols // LANES):
        out_ref[pl.ds(block * rows, rows), :] = acc_ref[:, pl.ds(block * LANES, LANES)].astype(BF16)
    used = rows * cols // LANES
    if used < out_ref.shape[0]:
        out_ref[pl.ds(used, out_ref.shape[0] - used), :] = jnp.zeros((out_ref.shape[0] - used, LANES), BF16)


RING = ((0, 0), (1, 0), (7, 0), (2, 0), (6, 0), (3, 0), (5, 0), (4, 0), (4, 64))


def ring_blocks(rows):
    count = lax.axis_size("shard")
    right = [(i, (i + 1) % count) for i in range(count)]
    left = [(i, (i - 1) % count) for i in range(count)]
    blocks = [rows]
    came_right = came_left = rows
    for _ in range(count // 2 - 1):
        came_right = lax.ppermute(came_right, "shard", right)
        came_left = lax.ppermute(came_left, "shard", left)
        blocks += [came_right, came_left]
    half = rows.shape[0] // 2
    blocks.append(lax.ppermute(came_right[:half], "shard", right))
    blocks.append(lax.ppermute(came_left[half:], "shard", left))
    return blocks


def local_term(saved_cols, keys, shard, tall):
    rows = saved_cols.shape[2]
    cols = keys[0].shape[1]
    vmem = pl.BlockSpec(memory_space=pltpu.VMEM)
    return pl.pallas_call(
        term_kernel,
        in_specs=[pl.BlockSpec(memory_space=pltpu.SMEM)] + [vmem] * (1 + len(keys)),
        out_specs=vmem,
        out_shape=jax.ShapeDtypeStruct((tall, LANES), BF16),
        scratch_shapes=[pltpu.VMEM((rows, cols), F32)],
        name="local_term",
    )(shard, saved_cols, *keys)


def sum_kernel(got_ref, out_ref):
    total = jnp.sum(got_ref[...].astype(F32), 0).astype(BF16)
    out_ref[...] = jnp.broadcast_to(total[None], out_ref.shape)


def sum_pieces(got):
    return pl.pallas_call(sum_kernel, out_shape=jax.ShapeDtypeStruct(got.shape, BF16), name="sum_pieces")(got)


def spread_kernel(full_ref, scale_ref, out_ref):
    rows, cols = out_ref.shape
    scale = scale_ref[...]
    for block in range(cols // LANES):
        out_ref[:, pl.ds(block * LANES, LANES)] = full_ref[pl.ds(block * rows, rows), :].astype(F32) * scale


def spread(full, scale, rows, cols):
    return pl.pallas_call(spread_kernel, out_shape=jax.ShapeDtypeStruct((rows, cols), F32), name="spread")(full, scale)


def window_kernel(
    weight_ref, acts_ref, came_fwd_ref, saved_ref, grads_ref, came_bwd_ref, key_grad_ref, gain_ref, cos_ref, sin_ref,
    place_ref, keys_ref, grad_out_ref, normed_ref, proj_ref, ng_ref,
):
    step = pl.program_id(0)
    block = weight_ref.shape[0]
    span = pl.ds(pl.multiple_of(step * block, block), block)

    @pl.when(step == 0)
    def _():
        stream = jnp.where(place_ref[0] == 0, acts_ref[...], came_fwd_ref[...]).astype(F32)
        inverse = lax.rsqrt(jnp.mean(stream * stream, -1, keepdims=True) + EPS)
        normed_ref[...] = (stream * inverse * gain_ref[...]).astype(BF16)
        proj_ref[...] = jnp.zeros_like(proj_ref)

    rows = weight_ref[...]
    proj_ref[...] += jnp.dot(normed_ref[:, span], rows, preferred_element_type=F32)
    ng_ref[:, span] = (
        lax.dot_general(key_grad_ref[...], rows, (((1,), (1,)), ((), ())), preferred_element_type=F32)
        * gain_ref[:, span]
    )

    @pl.when(step == pl.num_programs(0) - 1)
    def _():
        cosine = cos_ref[...]
        sine_part = sin_ref[...]
        for start in range(0, keys_ref.shape[1], HEAD):
            head = pl.ds(start, HEAD)
            keys_ref[:, head] = turn(proj_ref[:, head], cosine, sine_part).astype(BF16)
        saved = saved_ref[...].astype(F32)
        inverse = lax.rsqrt(jnp.mean(saved * saved, -1, keepdims=True) + EPS)
        scaled = ng_ref[...]
        pull = inverse * inverse * inverse * jnp.mean(saved * scaled, -1, keepdims=True)
        arrived = jnp.where(place_ref[1] == 0, grads_ref[...], came_bwd_ref[...]).astype(F32)
        grad_out_ref[...] = (arrived + (inverse * scaled - saved * pull)).astype(BF16)


def window(weight, acts, came_fwd, saved, grads, came_bwd, key_grad, gain_row, cosine, sine_part, place):
    tokens, width = acts.shape
    cols = weight.shape[2]
    block = width // weight.shape[0]
    whole = lambda *shape: pl.BlockSpec(shape, lambda i: (0,) * len(shape))
    return pl.pallas_call(
        window_kernel,
        grid=(width // block,),
        in_specs=[
            pl.BlockSpec((None, block, cols), lambda i: (i, 0, 0)),
            whole(tokens, width), whole(tokens, width), whole(tokens, width), whole(tokens, width), whole(tokens, width),
            whole(tokens, cols), whole(1, width), whole(tokens, HEAD), whole(tokens, HEAD),
            pl.BlockSpec(memory_space=pltpu.SMEM),
        ],
        out_specs=(whole(tokens, cols), whole(tokens, width)),
        out_shape=(jax.ShapeDtypeStruct((tokens, cols), BF16), jax.ShapeDtypeStruct((tokens, width), BF16)),
        scratch_shapes=[pltpu.VMEM((tokens, width), BF16), pltpu.VMEM((tokens, cols), F32), pltpu.VMEM((tokens, width), F32)],
        name="window",
    )(weight, acts, came_fwd, saved, grads, came_bwd, key_grad, gain_row, cosine, sine_part, place)


def per_device(acts_fwd, pos_fwd, saved_acts, pos_bwd, grads_in, key_cotan, weight, gain):
    section_pos = lax.axis_index("section")
    section_count = lax.axis_size("section")
    shard_count = lax.axis_size("shard")
    replica_count = lax.axis_size("replica")
    _, tok_rows, _ = saved_acts.shape
    own_rows, cols = weight.shape[1:]
    gain_row = gain[0]
    pieces = saved_acts[0].reshape(tok_rows, shard_count, own_rows).transpose(1, 0, 2)
    saved_cols = lax.all_to_all(pieces, "shard", split_axis=0, concat_axis=0)
    cos_b, sin_b = rope_tables(pos_bwd[0])
    key_grad, own_keys = key_factors(saved_acts[0], key_cotan[0], cos_b, sin_b)
    ring_keys = ring_blocks(own_keys)
    share = -(-own_rows // (replica_count * 8)) * 8
    padded = jnp.pad(weight[0], ((0, share * replica_count - own_rows), (0, 0)))
    mine = lax.dynamic_slice(padded, (lax.axis_index("replica") * share, 0), (share, cols))
    gathered = lax.all_gather(mine, ("shard", "replica"), axis=0, tiled=True)
    gathered = gathered.reshape(shard_count, share * replica_count, cols)
    total = own_rows * cols // LANES
    piece = -(-total // (replica_count * 8)) * 8
    shard = lax.axis_index("shard").astype(jnp.int32)[None]
    tall = local_term(saved_cols, ring_keys, shard, piece * replica_count)
    got = lax.all_to_all(tall.reshape(replica_count, piece, LANES), "replica", split_axis=0, concat_axis=0)
    own = sum_pieces(got)
    full = lax.all_to_all(own, "replica", split_axis=0, concat_axis=0).reshape(-1, LANES)
    token_total = tok_rows * shard_count * replica_count
    own_gain = lax.dynamic_slice(gain_row, (lax.axis_index("shard") * own_rows,), (own_rows,))
    scale = jnp.broadcast_to((own_gain * float(token_total) ** (-0.5))[:, None], (own_rows, LANES))
    weight_grad = spread(full, scale, own_rows, cols)
    came_fwd = from_behind(acts_fwd[0], "section", 1)
    came_bwd = from_behind(grads_in[0], "section", -1)
    cos_f, sin_f = rope_tables(pos_fwd[0])
    place = jnp.stack([section_pos, section_count - 1 - section_pos]).astype(jnp.int32)
    keys, grad_out = window(
        gathered, acts_fwd[0], came_fwd, saved_acts[0], grads_in[0], came_bwd, key_grad, gain_row[None], cos_f, sin_f, place
    )
    return (keys[None], grad_out[None], weight_grad[None])


def solution(mesh):
    rows3 = P("section", ("shard", "replica"), None)
    rows2 = P("section", ("shard", "replica"))

    return jax.shard_map(
        per_device,
        mesh=mesh,
        in_specs=(rows3, rows2, rows3, rows2, rows3, rows3, P("section", "shard", None), P("section", None)),
        out_specs=(rows3, rows3, P("section", "shard", None)),
        check_vma=False,
    )
```

```python
import jax
import jax.numpy as jnp
from jax import lax
from jax.experimental import pallas as pl
from jax.experimental.pallas import tpu as pltpu
from jax.sharding import PartitionSpec as P


HEAD = 128
LANES = 128
EPS = 1e-05
F32 = jnp.float32
BF16 = jnp.bfloat16


def from_behind(x, axis, by):
    size = lax.axis_size(axis)
    pairs = [(i, i + by) for i in range(size) if 0 <= i + by < size]
    return lax.ppermute(x, axis, pairs)


def rope_tables(positions):
    index = jnp.arange(HEAD // 2, dtype=F32)
    rate = 500000.0 ** (-(2.0 * index) / HEAD)
    rate = jnp.concatenate([rate, rate])
    sign = jnp.where(jnp.arange(HEAD) < HEAD // 2, -1.0, 1.0).astype(F32)
    angle = positions.astype(F32)[:, None] * rate[None, :]
    return jnp.cos(angle), jnp.sin(angle) * sign[None, :]


def turn(head, cosine, sine_part):
    return head * cosine + pltpu.roll(head, HEAD // 2, 1) * sine_part


def pieces_kernel(rows_ref, out_ref):
    out_ref[...] = rows_ref[...]


def column_pieces(rows, count):
    tokens, width = rows.shape
    each = width // count
    return pl.pallas_call(
        pieces_kernel,
        grid=(count,),
        in_specs=[pl.BlockSpec((tokens, each), lambda i: (0, i))],
        out_specs=pl.BlockSpec((None, tokens, each), lambda i: (i, 0, 0)),
        out_shape=jax.ShapeDtypeStruct((count, tokens, each), rows.dtype),
        name="column_pieces",
    )(rows)


def keys_kernel(saved_ref, cotan_ref, cos_ref, sin_ref, grad_ref, scaled_ref):
    saved = saved_ref[...].astype(F32)
    inverse = lax.rsqrt(jnp.mean(saved * saved, -1, keepdims=True) + EPS)
    cosine = cos_ref[...]
    sine_part = -sin_ref[...]
    for start in range(0, cotan_ref.shape[1], HEAD):
        span = pl.ds(start, HEAD)
        turned = turn(cotan_ref[:, span].astype(F32), cosine, sine_part)
        grad_ref[:, span] = turned.astype(BF16)
        scaled_ref[:, span] = (turned * inverse).astype(BF16)


def key_factors(saved, cotan, cosine, sine_part):
    shape = jax.ShapeDtypeStruct(cotan.shape, BF16)
    return pl.pallas_call(keys_kernel, out_shape=(shape, shape), name="key_factors")(saved, cotan, cosine, sine_part)


def term_kernel(shard_ref, saved_ref, *rest):
    *key_refs, out_ref, all_keys_ref = rest
    count, tokens, rows = saved_ref.shape
    cols = all_keys_ref.shape[1]
    for place, key_ref in enumerate(key_refs):
        distance, first = RING[place]
        block = lax.rem(shard_ref[0] + count - distance, count)
        start = pl.multiple_of(block * tokens + first, HEAD // 2)
        all_keys_ref[pl.ds(start, key_ref.shape[0]), :] = key_ref[...]
    term = lax.dot_general(
        saved_ref[...].reshape(count * tokens, rows), all_keys_ref[...], (((0,), (0,)), ((), ())),
        preferred_element_type=F32,
    )
    for block in range(cols // LANES):
        out_ref[pl.ds(block * rows, rows), :] = term[:, block * LANES : (block + 1) * LANES].astype(BF16)
    used = rows * cols // LANES
    if used < out_ref.shape[0]:
        out_ref[pl.ds(used, out_ref.shape[0] - used), :] = jnp.zeros((out_ref.shape[0] - used, LANES), BF16)


RING = ((0, 0), (1, 0), (7, 0), (2, 0), (6, 0), (3, 0), (5, 0), (4, 0), (4, 64))


def ring_blocks(rows):
    count = lax.axis_size("shard")
    right = [(i, (i + 1) % count) for i in range(count)]
    left = [(i, (i - 1) % count) for i in range(count)]
    blocks = [rows]
    came_right = came_left = rows
    for _ in range(count // 2 - 1):
        came_right = lax.ppermute(came_right, "shard", right)
        came_left = lax.ppermute(came_left, "shard", left)
        blocks += [came_right, came_left]
    half = rows.shape[0] // 2
    blocks.append(lax.ppermute(came_right[:half], "shard", right))
    blocks.append(lax.ppermute(came_left[half:], "shard", left))
    return blocks


def local_term(saved_cols, keys, shard, tall):
    cols = keys[0].shape[1]
    vmem = pl.BlockSpec(memory_space=pltpu.VMEM)
    return pl.pallas_call(
        term_kernel,
        in_specs=[pl.BlockSpec(memory_space=pltpu.SMEM)] + [vmem] * (1 + len(keys)),
        out_specs=vmem,
        out_shape=jax.ShapeDtypeStruct((tall, LANES), BF16),
        scratch_shapes=[pltpu.VMEM((saved_cols.shape[0] * saved_cols.shape[1], cols), BF16)],
        name="local_term",
    )(shard, saved_cols, *keys)


def sum_pieces(got):
    total = jnp.sum(got.astype(F32), 0).astype(BF16)
    return jnp.broadcast_to(total[None], got.shape)


def spread_kernel(full_ref, scale_ref, out_ref):
    rows, cols = out_ref.shape
    scale = scale_ref[...]
    for block in range(cols // LANES):
        out_ref[:, pl.ds(block * LANES, LANES)] = full_ref[pl.ds(block * rows, rows), :].astype(F32) * scale


def spread(full, scale, rows, cols):
    return pl.pallas_call(spread_kernel, out_shape=jax.ShapeDtypeStruct((rows, cols), F32), name="spread")(full, scale)


def window_kernel(
    weight_ref, acts_ref, came_fwd_ref, saved_ref, grads_ref, came_bwd_ref, key_grad_ref, gain_ref, cos_ref, sin_ref,
    place_ref, keys_ref, grad_out_ref, normed_ref, proj_ref, ng_ref,
):
    step = pl.program_id(0)
    block = weight_ref.shape[0]
    span = pl.ds(pl.multiple_of(step * block, block), block)

    @pl.when(step == 0)
    def _():
        stream = jnp.where(place_ref[0] == 0, acts_ref[...], came_fwd_ref[...]).astype(F32)
        inverse = lax.rsqrt(jnp.mean(stream * stream, -1, keepdims=True) + EPS)
        normed_ref[...] = (stream * inverse * gain_ref[...]).astype(BF16)
        proj_ref[...] = jnp.zeros_like(proj_ref)

    rows = weight_ref[...]
    proj_ref[...] += jnp.dot(normed_ref[:, span], rows, preferred_element_type=F32)
    ng_ref[:, span] = (
        lax.dot_general(key_grad_ref[...], rows, (((1,), (1,)), ((), ())), preferred_element_type=F32)
        * gain_ref[:, span]
    )

    @pl.when(step == pl.num_programs(0) - 1)
    def _():
        cosine = cos_ref[...]
        sine_part = sin_ref[...]
        for start in range(0, keys_ref.shape[1], HEAD):
            head = pl.ds(start, HEAD)
            keys_ref[:, head] = turn(proj_ref[:, head], cosine, sine_part).astype(BF16)
        saved = saved_ref[...].astype(F32)
        inverse = lax.rsqrt(jnp.mean(saved * saved, -1, keepdims=True) + EPS)
        scaled = ng_ref[...]
        pull = inverse * inverse * inverse * jnp.mean(saved * scaled, -1, keepdims=True)
        arrived = jnp.where(place_ref[1] == 0, grads_ref[...], came_bwd_ref[...]).astype(F32)
        grad_out_ref[...] = (arrived + (inverse * scaled - saved * pull)).astype(BF16)


def window(weight, acts, came_fwd, saved, grads, came_bwd, key_grad, gain_row, cosine, sine_part, place):
    tokens, width = acts.shape
    cols = weight.shape[2]
    block = width // weight.shape[0]
    whole = lambda *shape: pl.BlockSpec(shape, lambda i: (0,) * len(shape))
    return pl.pallas_call(
        window_kernel,
        grid=(width // block,),
        in_specs=[
            pl.BlockSpec((None, block, cols), lambda i: (i, 0, 0)),
            whole(tokens, width), whole(tokens, width), whole(tokens, width), whole(tokens, width), whole(tokens, width),
            whole(tokens, cols), whole(1, width), whole(tokens, HEAD), whole(tokens, HEAD),
            pl.BlockSpec(memory_space=pltpu.SMEM),
        ],
        out_specs=(whole(tokens, cols), whole(tokens, width)),
        out_shape=(jax.ShapeDtypeStruct((tokens, cols), BF16), jax.ShapeDtypeStruct((tokens, width), BF16)),
        scratch_shapes=[pltpu.VMEM((tokens, width), BF16), pltpu.VMEM((tokens, cols), F32), pltpu.VMEM((tokens, width), F32)],
        name="window",
    )(weight, acts, came_fwd, saved, grads, came_bwd, key_grad, gain_row, cosine, sine_part, place)


def per_device(acts_fwd, pos_fwd, saved_acts, pos_bwd, grads_in, key_cotan, weight, gain):
    section_pos = lax.axis_index("section")
    section_count = lax.axis_size("section")
    shard_count = lax.axis_size("shard")
    replica_count = lax.axis_size("replica")
    _, tok_rows, _ = saved_acts.shape
    own_rows, cols = weight.shape[1:]
    gain_row = gain[0]
    pieces = column_pieces(saved_acts[0], shard_count)
    saved_cols = lax.all_to_all(pieces, "shard", split_axis=0, concat_axis=0)
    cos_b, sin_b = rope_tables(pos_bwd[0])
    key_grad, own_keys = key_factors(saved_acts[0], key_cotan[0], cos_b, sin_b)
    ring_keys = ring_blocks(own_keys)
    gathered = lax.all_gather(weight[0], "shard", axis=0, tiled=True).reshape(shard_count, own_rows, cols)
    total = own_rows * cols // LANES
    piece = -(-total // (replica_count * 8)) * 8
    shard = lax.axis_index("shard").astype(jnp.int32)[None]
    tall = local_term(saved_cols, ring_keys, shard, piece * replica_count)
    got = lax.all_to_all(tall.reshape(replica_count, piece, LANES), "replica", split_axis=0, concat_axis=0)
    own = sum_pieces(got)
    full = lax.all_to_all(own, "replica", split_axis=0, concat_axis=0).reshape(-1, LANES)
    token_total = tok_rows * shard_count * replica_count
    own_gain = lax.dynamic_slice(gain_row, (lax.axis_index("shard") * own_rows,), (own_rows,))
    scale = jnp.broadcast_to((own_gain * float(token_total) ** (-0.5))[:, None], (own_rows, LANES))
    weight_grad = spread(full, scale, own_rows, cols)
    came_fwd = from_behind(acts_fwd[0], "section", 1)
    came_bwd = from_behind(grads_in[0], "section", -1)
    cos_f, sin_f = rope_tables(pos_fwd[0])
    place = jnp.stack([section_pos, section_count - 1 - section_pos]).astype(jnp.int32)
    keys, grad_out = window(
        gathered, acts_fwd[0], came_fwd, saved_acts[0], grads_in[0], came_bwd, key_grad, gain_row[None], cos_f, sin_f, place
    )
    return (keys[None], grad_out[None], weight_grad[None])


def solution(mesh):
    rows3 = P("section", ("shard", "replica"), None)
    rows2 = P("section", ("shard", "replica"))

    return jax.shard_map(
        per_device,
        mesh=mesh,
        in_specs=(rows3, rows2, rows3, rows2, rows3, rows3, P("section", "shard", None), P("section", None)),
        out_specs=(rows3, rows3, P("section", "shard", None)),
        check_vma=False,
    )
```

```python
import jax
import jax.numpy as jnp
from jax import lax
from jax.experimental import pallas as pl
from jax.experimental.pallas import tpu as pltpu
from jax.sharding import PartitionSpec as P


HEAD = 128
LANES = 128
EPS = 1e-05
F32 = jnp.float32
BF16 = jnp.bfloat16


def from_behind(x, axis, by):
    size = lax.axis_size(axis)
    pairs = [(i, i + by) for i in range(size) if 0 <= i + by < size]
    return lax.ppermute(x, axis, pairs)


def rope_tables(positions):
    index = jnp.arange(HEAD // 2, dtype=F32)
    rate = 500000.0 ** (-(2.0 * index) / HEAD)
    rate = jnp.concatenate([rate, rate])
    sign = jnp.where(jnp.arange(HEAD) < HEAD // 2, -1.0, 1.0).astype(F32)
    angle = positions.astype(F32)[:, None] * rate[None, :]
    return jnp.cos(angle), jnp.sin(angle) * sign[None, :]


def turn(head, cosine, sine_part):
    return head * cosine + pltpu.roll(head, HEAD // 2, 1) * sine_part


def keys_kernel(saved_ref, cotan_ref, cos_ref, sin_ref, grad_ref, scaled_ref):
    saved = saved_ref[...].astype(F32)
    inverse = lax.rsqrt(jnp.mean(saved * saved, -1, keepdims=True) + EPS)
    cosine = cos_ref[...]
    sine_part = -sin_ref[...]
    for start in range(0, cotan_ref.shape[1], HEAD):
        span = pl.ds(start, HEAD)
        turned = turn(cotan_ref[:, span].astype(F32), cosine, sine_part)
        grad_ref[:, span] = turned.astype(BF16)
        scaled_ref[:, span] = (turned * inverse).astype(BF16)


def key_factors(saved, cotan, cosine, sine_part):
    shape = jax.ShapeDtypeStruct(cotan.shape, BF16)
    return pl.pallas_call(keys_kernel, out_shape=(shape, shape), name="key_factors")(saved, cotan, cosine, sine_part)


def tall_pieces(term, count):
    rows, cols = term.shape
    tall = term.astype(BF16).reshape(rows, cols // LANES, LANES).transpose(1, 0, 2).reshape(-1, LANES)
    piece = -(-tall.shape[0] // (count * 8)) * 8
    return jnp.pad(tall, ((0, piece * count - tall.shape[0]), (0, 0))).reshape(count, piece, LANES)


def sum_pieces(got):
    total = jnp.sum(got.astype(F32), 0).astype(BF16)
    return jnp.broadcast_to(total[None], got.shape)


def from_tall(full, rows, cols):
    full = full.reshape(-1, LANES)[: rows * cols // LANES].astype(F32)
    return full.reshape(cols // LANES, rows, LANES).transpose(1, 0, 2).reshape(rows, cols)


def window_kernel(
    weight_ref, acts_ref, came_fwd_ref, saved_ref, grads_ref, came_bwd_ref, key_grad_ref, gain_ref, cos_ref, sin_ref,
    place_ref, keys_ref, grad_out_ref, normed_ref, proj_ref, ng_ref,
):
    step = pl.program_id(0)
    block = weight_ref.shape[0]
    span = pl.ds(pl.multiple_of(step * block, block), block)

    @pl.when(step == 0)
    def _():
        stream = jnp.where(place_ref[0] == 0, acts_ref[...], came_fwd_ref[...]).astype(F32)
        inverse = lax.rsqrt(jnp.mean(stream * stream, -1, keepdims=True) + EPS)
        normed_ref[...] = (stream * inverse * gain_ref[...]).astype(BF16)
        proj_ref[...] = jnp.zeros_like(proj_ref)

    rows = weight_ref[...]
    proj_ref[...] += jnp.dot(normed_ref[:, span], rows, preferred_element_type=F32)
    ng_ref[:, span] = (
        lax.dot_general(key_grad_ref[...], rows, (((1,), (1,)), ((), ())), preferred_element_type=F32)
        * gain_ref[:, span]
    )

    @pl.when(step == pl.num_programs(0) - 1)
    def _():
        cosine = cos_ref[...]
        sine_part = sin_ref[...]
        for start in range(0, keys_ref.shape[1], HEAD):
            head = pl.ds(start, HEAD)
            keys_ref[:, head] = turn(proj_ref[:, head], cosine, sine_part).astype(BF16)
        saved = saved_ref[...].astype(F32)
        inverse = lax.rsqrt(jnp.mean(saved * saved, -1, keepdims=True) + EPS)
        scaled = ng_ref[...]
        pull = inverse * inverse * inverse * jnp.mean(saved * scaled, -1, keepdims=True)
        arrived = jnp.where(place_ref[1] == 0, grads_ref[...], came_bwd_ref[...]).astype(F32)
        grad_out_ref[...] = (arrived + (inverse * scaled - saved * pull)).astype(BF16)


def window(weight, acts, came_fwd, saved, grads, came_bwd, key_grad, gain_row, cosine, sine_part, place):
    tokens, width = acts.shape
    cols = weight.shape[2]
    block = width // weight.shape[0]
    whole = lambda *shape: pl.BlockSpec(shape, lambda i: (0,) * len(shape))
    return pl.pallas_call(
        window_kernel,
        grid=(width // block,),
        in_specs=[
            pl.BlockSpec((None, block, cols), lambda i: (i, 0, 0)),
            whole(tokens, width), whole(tokens, width), whole(tokens, width), whole(tokens, width), whole(tokens, width),
            whole(tokens, cols), whole(1, width), whole(tokens, HEAD), whole(tokens, HEAD),
            pl.BlockSpec(memory_space=pltpu.SMEM),
        ],
        out_specs=(whole(tokens, cols), whole(tokens, width)),
        out_shape=(jax.ShapeDtypeStruct((tokens, cols), BF16), jax.ShapeDtypeStruct((tokens, width), BF16)),
        scratch_shapes=[pltpu.VMEM((tokens, width), BF16), pltpu.VMEM((tokens, cols), F32), pltpu.VMEM((tokens, width), F32)],
        name="window",
    )(weight, acts, came_fwd, saved, grads, came_bwd, key_grad, gain_row, cosine, sine_part, place)


def per_device(acts_fwd, pos_fwd, saved_acts, pos_bwd, grads_in, key_cotan, weight, gain):
    section_pos = lax.axis_index("section")
    section_count = lax.axis_size("section")
    shard_count = lax.axis_size("shard")
    replica_count = lax.axis_size("replica")
    _, tok_rows, _ = saved_acts.shape
    own_rows, cols = weight.shape[1:]
    gain_row = gain[0]
    pieces = saved_acts[0].reshape(tok_rows, shard_count, own_rows).transpose(1, 0, 2)
    saved_cols = lax.all_to_all(pieces, "shard", split_axis=0, concat_axis=0)
    saved_cols = saved_cols.reshape(shard_count * tok_rows, own_rows)
    cos_b, sin_b = rope_tables(pos_bwd[0])
    key_grad, own_keys = key_factors(saved_acts[0], key_cotan[0], cos_b, sin_b)
    scaled_keys = lax.all_gather(own_keys, "shard", axis=0, tiled=True)
    gathered = lax.all_gather(weight[0], "shard", axis=0, tiled=True).reshape(shard_count, own_rows, cols)
    term = lax.dot_general(saved_cols, scaled_keys, (((0,), (0,)), ((), ())), preferred_element_type=F32)
    got = lax.all_to_all(tall_pieces(term, replica_count), "replica", split_axis=0, concat_axis=0)
    own = sum_pieces(got)
    full = lax.all_to_all(own, "replica", split_axis=0, concat_axis=0)
    token_total = tok_rows * shard_count * replica_count
    own_gain = lax.dynamic_slice(gain_row, (lax.axis_index("shard") * own_rows,), (own_rows,))
    scale = own_gain * float(token_total) ** (-0.5)
    weight_grad = from_tall(full, own_rows, cols) * scale[:, None]
    came_fwd = from_behind(acts_fwd[0], "section", 1)
    came_bwd = from_behind(grads_in[0], "section", -1)
    cos_f, sin_f = rope_tables(pos_fwd[0])
    place = jnp.stack([section_pos, section_count - 1 - section_pos]).astype(jnp.int32)
    keys, grad_out = window(
        gathered, acts_fwd[0], came_fwd, saved_acts[0], grads_in[0], came_bwd, key_grad, gain_row[None], cos_f, sin_f, place
    )
    return (keys[None], grad_out[None], weight_grad[None])


def solution(mesh):
    rows3 = P("section", ("shard", "replica"), None)
    rows2 = P("section", ("shard", "replica"))

    return jax.shard_map(
        per_device,
        mesh=mesh,
        in_specs=(rows3, rows2, rows3, rows2, rows3, rows3, P("section", "shard", None), P("section", None)),
        out_specs=(rows3, rows3, P("section", "shard", None)),
        check_vma=False,
    )
```

```python
import jax
import jax.numpy as jnp
from jax import lax
from jax.experimental import pallas as pl
from jax.experimental.pallas import tpu as pltpu
from jax.sharding import PartitionSpec as P


HEAD = 128
LANES = 128
EPS = 1e-05
F32 = jnp.float32
BF16 = jnp.bfloat16


def from_behind(x, axis, by):
    size = lax.axis_size(axis)
    pairs = [(i, i + by) for i in range(size) if 0 <= i + by < size]
    return lax.ppermute(x, axis, pairs)


def rope_tables(positions):
    index = jnp.arange(HEAD // 2, dtype=F32)
    rate = 500000.0 ** (-(2.0 * index) / HEAD)
    rate = jnp.concatenate([rate, rate])
    sign = jnp.where(jnp.arange(HEAD) < HEAD // 2, -1.0, 1.0).astype(F32)
    angle = positions.astype(F32)[:, None] * rate[None, :]
    return jnp.cos(angle), jnp.sin(angle) * sign[None, :]


def turn(head, cosine, sine_part):
    return head * cosine + pltpu.roll(head, HEAD // 2, 1) * sine_part


def keys_kernel(saved_ref, cotan_ref, cos_ref, sin_ref, grad_ref, scaled_ref):
    saved = saved_ref[...].astype(F32)
    inverse = lax.rsqrt(jnp.mean(saved * saved, -1, keepdims=True) + EPS)
    cosine = cos_ref[...]
    sine_part = -sin_ref[...]
    for start in range(0, cotan_ref.shape[1], HEAD):
        span = pl.ds(start, HEAD)
        turned = turn(cotan_ref[:, span].astype(F32), cosine, sine_part)
        grad_ref[:, span] = turned.astype(BF16)
        scaled_ref[:, span] = (turned * inverse).astype(BF16)


def key_factors(saved, cotan, cosine, sine_part):
    shape = jax.ShapeDtypeStruct(cotan.shape, BF16)
    return pl.pallas_call(keys_kernel, out_shape=(shape, shape), name="key_factors")(saved, cotan, cosine, sine_part)


def tall_pieces(term, count):
    rows, cols = term.shape
    tall = term.astype(BF16).reshape(rows, cols // LANES, LANES).transpose(1, 0, 2).reshape(-1, LANES)
    piece = -(-tall.shape[0] // (count * 8)) * 8
    return jnp.pad(tall, ((0, piece * count - tall.shape[0]), (0, 0))).reshape(count, piece, LANES)


def sum_pieces(got):
    total = jnp.sum(got.astype(F32), 0).astype(BF16)
    return jnp.broadcast_to(total[None], got.shape)


def from_tall(full, rows, cols):
    full = full.reshape(-1, LANES)[: rows * cols // LANES].astype(F32)
    return full.reshape(cols // LANES, rows, LANES).transpose(1, 0, 2).reshape(rows, cols)


def streams_kernel(acts_ref, came_fwd_ref, grads_ref, came_bwd_ref, saved_ref, gain_ref, place_ref, normed_ref, arrived_ref, inverse_ref):
    stream = jnp.where(place_ref[0] == 0, acts_ref[...], came_fwd_ref[...]).astype(F32)
    inverse = lax.rsqrt(jnp.mean(stream * stream, -1, keepdims=True) + EPS)
    normed_ref[...] = (stream * inverse * gain_ref[...]).astype(BF16)
    arrived_ref[...] = jnp.where(place_ref[1] == 0, grads_ref[...], came_bwd_ref[...])
    saved = saved_ref[...].astype(F32)
    inverse = lax.rsqrt(jnp.mean(saved * saved, -1, keepdims=True) + EPS)
    inverse_ref[...] = jnp.broadcast_to(inverse, inverse_ref.shape)


def streams(acts, came_fwd, grads, came_bwd, saved, gain_row, place):
    tokens, width = acts.shape
    group = 32
    rows = pl.BlockSpec((group, width), lambda i: (i, 0))
    return pl.pallas_call(
        streams_kernel,
        grid=(tokens // group,),
        in_specs=[rows] * 5 + [pl.BlockSpec((1, width), lambda i: (0, 0)), pl.BlockSpec(memory_space=pltpu.SMEM)],
        out_specs=(rows, rows, pl.BlockSpec((group, LANES), lambda i: (i, 0))),
        out_shape=(
            jax.ShapeDtypeStruct((tokens, width), BF16),
            jax.ShapeDtypeStruct((tokens, width), BF16),
            jax.ShapeDtypeStruct((tokens, LANES), F32),
        ),
        name="streams",
    )(acts, came_fwd, grads, came_bwd, saved, gain_row, place)


def window_kernel(
    weight_ref, normed_ref, saved_ref, arrived_ref, key_grad_ref, gain_ref, inverse_ref, cos_ref, sin_ref,
    keys_ref, grad_out_ref, proj_ref, scaled_ref, pull_ref,
):
    finish = pl.program_id(0)
    step = pl.program_id(1)
    block = weight_ref.shape[0]
    width = block * pl.num_programs(1)

    @pl.when(finish == 0)
    def _():
        rows = weight_ref[...]
        part = jnp.dot(normed_ref[...], rows, preferred_element_type=F32)
        scaled = (
            lax.dot_general(key_grad_ref[...], rows, (((1,), (1,)), ((), ())), preferred_element_type=F32)
            * gain_ref[...]
        )
        scaled_ref[step] = scaled
        pull = jnp.broadcast_to(jnp.sum(saved_ref[...].astype(F32) * scaled, -1, keepdims=True), pull_ref.shape)

        @pl.when(step == 0)
        def _():
            proj_ref[...] = part
            pull_ref[...] = pull

        @pl.when(step > 0)
        def _():
            proj_ref[...] += part
            pull_ref[...] += pull

    @pl.when(finish == 1)
    def _():
        @pl.when(step == 0)
        def _():
            cosine = cos_ref[...]
            sine_part = sin_ref[...]
            for start in range(0, keys_ref.shape[1], HEAD):
                head = pl.ds(start, HEAD)
                keys_ref[:, head] = turn(proj_ref[:, head], cosine, sine_part).astype(BF16)

        inverse = inverse_ref[:, :1]
        pull = inverse * inverse * inverse * (pull_ref[:, :1] / width)
        grad = inverse * scaled_ref[step] - saved_ref[...].astype(F32) * pull
        grad_out_ref[...] = (arrived_ref[...].astype(F32) + grad).astype(BF16)


def window(weight, normed, saved, arrived, key_grad, gain_row, inverse, cosine, sine_part):
    tokens, width = normed.shape
    cols = weight.shape[1]
    steps = 4
    block = width // steps
    whole = lambda *shape: pl.BlockSpec(shape, lambda p, i: (0,) * len(shape))
    first = lambda p, i: i + p * (steps - 1 - i)
    last = lambda p, i: p * i
    return pl.pallas_call(
        window_kernel,
        grid=(2, steps),
        in_specs=[
            pl.BlockSpec((block, cols), lambda p, i: (first(p, i), 0)),
            pl.BlockSpec((tokens, block), lambda p, i: (0, first(p, i))),
            pl.BlockSpec((tokens, block), lambda p, i: (0, i)),
            pl.BlockSpec((tokens, block), lambda p, i: (0, last(p, i))),
            whole(tokens, cols),
            pl.BlockSpec((1, block), lambda p, i: (0, first(p, i))),
            whole(tokens, LANES), whole(tokens, HEAD), whole(tokens, HEAD),
        ],
        out_specs=(whole(tokens, cols), pl.BlockSpec((tokens, block), lambda p, i: (0, last(p, i)))),
        out_shape=(jax.ShapeDtypeStruct((tokens, cols), BF16), jax.ShapeDtypeStruct((tokens, width), BF16)),
        scratch_shapes=[
            pltpu.VMEM((tokens, cols), F32), pltpu.VMEM((steps, tokens, block), F32), pltpu.VMEM((tokens, LANES), F32)
        ],
        name="window",
    )(weight, normed, saved, arrived, key_grad, gain_row, inverse, cosine, sine_part)


def per_device(acts_fwd, pos_fwd, saved_acts, pos_bwd, grads_in, key_cotan, weight, gain):
    section_pos = lax.axis_index("section")
    section_count = lax.axis_size("section")
    shard_count = lax.axis_size("shard")
    replica_count = lax.axis_size("replica")
    _, tok_rows, _ = saved_acts.shape
    own_rows, cols = weight.shape[1:]
    gain_row = gain[0]
    pieces = saved_acts[0].reshape(tok_rows, shard_count, own_rows).transpose(1, 0, 2)
    saved_cols = lax.all_to_all(pieces, "shard", split_axis=0, concat_axis=0)
    saved_cols = saved_cols.reshape(shard_count * tok_rows, own_rows)
    cos_b, sin_b = rope_tables(pos_bwd[0])
    key_grad, own_keys = key_factors(saved_acts[0], key_cotan[0], cos_b, sin_b)
    scaled_keys = lax.all_gather(own_keys, "shard", axis=0, tiled=True)
    gathered = lax.all_gather(weight[0], "shard", axis=0, tiled=True)
    term = lax.dot_general(saved_cols, scaled_keys, (((0,), (0,)), ((), ())), preferred_element_type=F32)
    got = lax.all_to_all(tall_pieces(term, replica_count), "replica", split_axis=0, concat_axis=0)
    own = sum_pieces(got)
    full = lax.all_to_all(own, "replica", split_axis=0, concat_axis=0)
    token_total = tok_rows * shard_count * replica_count
    own_gain = lax.dynamic_slice(gain_row, (lax.axis_index("shard") * own_rows,), (own_rows,))
    scale = own_gain * float(token_total) ** (-0.5)
    weight_grad = from_tall(full, own_rows, cols) * scale[:, None]
    came_fwd = from_behind(acts_fwd[0], "section", 1)
    came_bwd = from_behind(grads_in[0], "section", -1)
    cos_f, sin_f = rope_tables(pos_fwd[0])
    place = jnp.stack([section_pos, section_count - 1 - section_pos]).astype(jnp.int32)
    normed, arrived, inverse = streams(
        acts_fwd[0], came_fwd, grads_in[0], came_bwd, saved_acts[0], gain_row[None], place
    )
    keys, grad_out = window(
        gathered, normed, saved_acts[0], arrived, key_grad, gain_row[None], inverse, cos_f, sin_f
    )
    return (keys[None], grad_out[None], weight_grad[None])


def solution(mesh):
    rows3 = P("section", ("shard", "replica"), None)
    rows2 = P("section", ("shard", "replica"))

    return jax.shard_map(
        per_device,
        mesh=mesh,
        in_specs=(rows3, rows2, rows3, rows2, rows3, rows3, P("section", "shard", None), P("section", None)),
        out_specs=(rows3, rows3, P("section", "shard", None)),
        check_vma=False,
    )
```

```python
import jax
import jax.numpy as jnp
from jax import lax
from jax.experimental import pallas as pl
from jax.experimental.pallas import tpu as pltpu
from jax.sharding import PartitionSpec as P


HEAD = 128
LANES = 128
EPS = 1e-05
F32 = jnp.float32
BF16 = jnp.bfloat16


def from_behind(x, axis, by):
    size = lax.axis_size(axis)
    pairs = [(i, i + by) for i in range(size) if 0 <= i + by < size]
    return lax.ppermute(x, axis, pairs)


def rope_tables(positions):
    index = jnp.arange(HEAD // 2, dtype=F32)
    rate = 500000.0 ** (-(2.0 * index) / HEAD)
    rate = jnp.concatenate([rate, rate])
    sign = jnp.where(jnp.arange(HEAD) < HEAD // 2, -1.0, 1.0).astype(F32)
    angle = positions.astype(F32)[:, None] * rate[None, :]
    return jnp.cos(angle), jnp.sin(angle) * sign[None, :]


def turn(head, cosine, sine_part):
    return head * cosine + pltpu.roll(head, HEAD // 2, 1) * sine_part


def keys_kernel(saved_ref, cotan_ref, cos_ref, sin_ref, grad_ref, scaled_ref):
    saved = saved_ref[...].astype(F32)
    inverse = lax.rsqrt(jnp.mean(saved * saved, -1, keepdims=True) + EPS)
    cosine = cos_ref[...]
    sine_part = -sin_ref[...]
    for start in range(0, cotan_ref.shape[1], HEAD):
        span = pl.ds(start, HEAD)
        turned = turn(cotan_ref[:, span].astype(F32), cosine, sine_part)
        grad_ref[:, span] = turned.astype(BF16)
        scaled_ref[:, span] = (turned * inverse).astype(BF16)


def key_factors(saved, cotan, cosine, sine_part):
    shape = jax.ShapeDtypeStruct(cotan.shape, BF16)
    group = 32
    rows = lambda array: pl.BlockSpec((group, array.shape[1]), lambda i: (i, 0))
    return pl.pallas_call(
        keys_kernel,
        grid=(cotan.shape[0] // group,),
        in_specs=[rows(saved), rows(cotan), rows(cosine), rows(sine_part)],
        out_specs=(rows(cotan), rows(cotan)),
        out_shape=(shape, shape),
        name="key_factors",
    )(saved, cotan, cosine, sine_part)


def tall_pieces(term, count):
    rows, cols = term.shape
    tall = term.astype(BF16).reshape(rows, cols // LANES, LANES).transpose(1, 0, 2).reshape(-1, LANES)
    piece = -(-tall.shape[0] // (count * 8)) * 8
    return jnp.pad(tall, ((0, piece * count - tall.shape[0]), (0, 0))).reshape(count, piece, LANES)


def sum_pieces(got):
    total = jnp.sum(got.astype(F32), 0).astype(BF16)
    return jnp.broadcast_to(total[None], got.shape)


def from_tall(full, rows, cols):
    full = full.reshape(-1, LANES)[: rows * cols // LANES].astype(F32)
    return full.reshape(cols // LANES, rows, LANES).transpose(1, 0, 2).reshape(rows, cols)


def streams_kernel(acts_ref, came_fwd_ref, grads_ref, came_bwd_ref, saved_ref, gain_ref, place_ref, normed_ref, arrived_ref, inverse_ref):
    stream = jnp.where(place_ref[0] == 0, acts_ref[...], came_fwd_ref[...]).astype(F32)
    inverse = lax.rsqrt(jnp.mean(stream * stream, -1, keepdims=True) + EPS)
    normed_ref[...] = (stream * inverse * gain_ref[...]).astype(BF16)
    arrived_ref[...] = jnp.where(place_ref[1] == 0, grads_ref[...], came_bwd_ref[...])
    saved = saved_ref[...].astype(F32)
    inverse = lax.rsqrt(jnp.mean(saved * saved, -1, keepdims=True) + EPS)
    inverse_ref[...] = jnp.broadcast_to(inverse, inverse_ref.shape)


def streams(acts, came_fwd, grads, came_bwd, saved, gain_row, place):
    tokens, width = acts.shape
    group = 32
    rows = pl.BlockSpec((group, width), lambda i: (i, 0))
    return pl.pallas_call(
        streams_kernel,
        grid=(tokens // group,),
        in_specs=[rows] * 5 + [pl.BlockSpec((1, width), lambda i: (0, 0)), pl.BlockSpec(memory_space=pltpu.SMEM)],
        out_specs=(rows, rows, pl.BlockSpec((group, LANES), lambda i: (i, 0))),
        out_shape=(
            jax.ShapeDtypeStruct((tokens, width), BF16),
            jax.ShapeDtypeStruct((tokens, width), BF16),
            jax.ShapeDtypeStruct((tokens, LANES), F32),
        ),
        name="streams",
    )(acts, came_fwd, grads, came_bwd, saved, gain_row, place)


def window_kernel(
    weight_ref, normed_ref, saved_ref, arrived_ref, key_grad_ref, gain_ref, inverse_ref, cos_ref, sin_ref,
    keys_ref, grad_out_ref, proj_ref, scaled_ref, pull_ref,
):
    finish = pl.program_id(0)
    step = pl.program_id(1)
    block = weight_ref.shape[0]
    width = block * pl.num_programs(1)

    @pl.when(finish == 0)
    def _():
        rows = weight_ref[...]
        part = jnp.dot(normed_ref[...], rows, preferred_element_type=F32)
        scaled = (
            lax.dot_general(key_grad_ref[...], rows, (((1,), (1,)), ((), ())), preferred_element_type=F32)
            * gain_ref[...]
        )
        scaled_ref[step] = scaled
        pull = jnp.broadcast_to(jnp.sum(saved_ref[...].astype(F32) * scaled, -1, keepdims=True), pull_ref.shape)

        @pl.when(step == 0)
        def _():
            proj_ref[...] = part
            pull_ref[...] = pull

        @pl.when(step > 0)
        def _():
            proj_ref[...] += part
            pull_ref[...] += pull

    @pl.when(finish == 1)
    def _():
        @pl.when(step == 0)
        def _():
            cosine = cos_ref[...]
            sine_part = sin_ref[...]
            for start in range(0, keys_ref.shape[1], HEAD):
                head = pl.ds(start, HEAD)
                keys_ref[:, head] = turn(proj_ref[:, head], cosine, sine_part).astype(BF16)

        inverse = inverse_ref[:, :1]
        pull = inverse * inverse * inverse * (pull_ref[:, :1] / width)
        grad = inverse * scaled_ref[step] - saved_ref[...].astype(F32) * pull
        grad_out_ref[...] = (arrived_ref[...].astype(F32) + grad).astype(BF16)


def window(weight, normed, saved, arrived, key_grad, gain_row, inverse, cosine, sine_part):
    tokens, width = normed.shape
    cols = weight.shape[1]
    steps = 4
    block = width // steps
    whole = lambda *shape: pl.BlockSpec(shape, lambda p, i: (0,) * len(shape))
    first = lambda p, i: i + p * (steps - 1 - i)
    last = lambda p, i: p * i
    return pl.pallas_call(
        window_kernel,
        grid=(2, steps),
        in_specs=[
            pl.BlockSpec((block, cols), lambda p, i: (first(p, i), 0)),
            pl.BlockSpec((tokens, block), lambda p, i: (0, first(p, i))),
            pl.BlockSpec((tokens, block), lambda p, i: (0, i)),
            pl.BlockSpec((tokens, block), lambda p, i: (0, last(p, i))),
            whole(tokens, cols),
            pl.BlockSpec((1, block), lambda p, i: (0, first(p, i))),
            whole(tokens, LANES), whole(tokens, HEAD), whole(tokens, HEAD),
        ],
        out_specs=(whole(tokens, cols), pl.BlockSpec((tokens, block), lambda p, i: (0, last(p, i)))),
        out_shape=(jax.ShapeDtypeStruct((tokens, cols), BF16), jax.ShapeDtypeStruct((tokens, width), BF16)),
        scratch_shapes=[
            pltpu.VMEM((tokens, cols), F32), pltpu.VMEM((steps, tokens, block), F32), pltpu.VMEM((tokens, LANES), F32)
        ],
        name="window",
    )(weight, normed, saved, arrived, key_grad, gain_row, inverse, cosine, sine_part)


def per_device(acts_fwd, pos_fwd, saved_acts, pos_bwd, grads_in, key_cotan, weight, gain):
    section_pos = lax.axis_index("section")
    section_count = lax.axis_size("section")
    shard_count = lax.axis_size("shard")
    replica_count = lax.axis_size("replica")
    _, tok_rows, _ = saved_acts.shape
    own_rows, cols = weight.shape[1:]
    gain_row = gain[0]
    pieces = saved_acts[0].reshape(tok_rows, shard_count, own_rows).transpose(1, 0, 2)
    saved_cols = lax.all_to_all(pieces, "shard", split_axis=0, concat_axis=0)
    saved_cols = saved_cols.reshape(shard_count * tok_rows, own_rows)
    cos_b, sin_b = rope_tables(pos_bwd[0])
    key_grad, own_keys = key_factors(saved_acts[0], key_cotan[0], cos_b, sin_b)
    scaled_keys = lax.all_gather(own_keys, "shard", axis=0, tiled=True)
    gathered = lax.all_gather(weight[0], "shard", axis=0, tiled=True)
    term = lax.dot_general(saved_cols, scaled_keys, (((0,), (0,)), ((), ())), preferred_element_type=F32)
    got = lax.all_to_all(tall_pieces(term, replica_count), "replica", split_axis=0, concat_axis=0)
    own = sum_pieces(got)
    full = lax.all_to_all(own, "replica", split_axis=0, concat_axis=0)
    token_total = tok_rows * shard_count * replica_count
    own_gain = lax.dynamic_slice(gain_row, (lax.axis_index("shard") * own_rows,), (own_rows,))
    scale = own_gain * float(token_total) ** (-0.5)
    weight_grad = from_tall(full, own_rows, cols) * scale[:, None]
    came_fwd = from_behind(acts_fwd[0], "section", 1)
    came_bwd = from_behind(grads_in[0], "section", -1)
    later, _ = lax.optimization_barrier((pos_fwd[0], key_grad))
    cos_f, sin_f = rope_tables(later)
    place = jnp.stack([section_pos, section_count - 1 - section_pos]).astype(jnp.int32)
    normed, arrived, inverse = streams(
        acts_fwd[0], came_fwd, grads_in[0], came_bwd, saved_acts[0], gain_row[None], place
    )
    keys, grad_out = window(
        gathered, normed, saved_acts[0], arrived, key_grad, gain_row[None], inverse, cos_f, sin_f
    )
    return (keys[None], grad_out[None], weight_grad[None])


def solution(mesh):
    rows3 = P("section", ("shard", "replica"), None)
    rows2 = P("section", ("shard", "replica"))

    return jax.shard_map(
        per_device,
        mesh=mesh,
        in_specs=(rows3, rows2, rows3, rows2, rows3, rows3, P("section", "shard", None), P("section", None)),
        out_specs=(rows3, rows3, P("section", "shard", None)),
        check_vma=False,
    )
```
